128 devices in a mesh: row: 16 (over x, z), col: 8 (over y, core).
Axes of the slice: x: 4, y: 4, z: 4, core: 2. Of those that a mesh axis runs over, the one named last changes fastest.
Arguments:
- coarse_kernel: bfloat16 [16, 16, 256, 256], P('col', 'row'), may hold values from -0.03125 to 0.03125
- correlations: bfloat16 [128, 256, 256], P('col'), may hold values from -0.375 to 0.375
- coarse_of: int32 [128], replicated, may hold values from 0 to 15
- energy: float32 [32768], P('row'), may hold values from 1 to 8
- start_vectors: float32 [32768, 64], P(('row', 'col')), may hold values from -6 to 6
Outputs:
- hamiltonian: bfloat16 [32768, 32768], P('row', 'col')
- vectors: float32 [32768, 64], P(('row', 'col'))
- gram: float32 [64, 64], replicated
The draws below stay inside these ranges and needn't reach their ends.
All inputs are finite; a program needn't handle non-finite values.
Results may differ from the reference program's by a relative error of at most 0.009.
Values may be sent and summed in bfloat16 or wider, within the bound.
A program may use at most 192 MiB of HBM per device.

```python
import math
import jax
import jax.numpy as jnp
from jax import lax

NK = 128
NKC = 16
VECS = 64
STEPS = 2
P_SIZE = 256
HAM = 32768


def with_ends(values, stream_key, least, top_value):
    index_at = [jax.random.randint(jax.random.fold_in(stream_key, axis), (), 0, length) for axis, length in enumerate(values.shape)]
    longest = values.shape.index(max(values.shape))
    neighbour = index_at[:longest] + [(index_at[longest] + 1) % values.shape[longest]] + index_at[longest + 1:]
    return values.at[tuple(index_at)].set(least).at[tuple(neighbour)].set(top_value)


def level_of(stream_key, dims, split, least, largest):
    level, own = 1.0, jax.random.fold_in(stream_key, 6)
    for position, parts in split:
        heights = jnp.exp(jax.random.uniform(jax.random.fold_in(own, position), (parts,), jnp.float32, least / len(split), largest / len(split)))
        level = level * jnp.repeat(heights, dims[position] // parts).reshape([-1 if axis == position else 1 for axis in range(len(dims))])
    return level


def noise(own_key, dims, deviation, bound, split=(), held_as=jnp.bfloat16):
    factor_of = level_of(own_key, dims, split, -0.22, 0.18) if split else 1.0
    array = jax.random.normal(own_key, dims, jnp.float32) * deviation * factor_of
    return jnp.minimum(jnp.maximum(array, -bound), bound).astype(held_as)


def setup_inputs(seed: int = 0) -> dict:
    seeds = jax.random.split(jax.random.key(seed), 6)
    return {
        "coarse_kernel": noise(seeds[0], (NKC, NKC, P_SIZE, P_SIZE), (NK * P_SIZE) ** -0.5, 0.03125, ((0, 8), (1, 16))),
        "correlations": noise(seeds[1], (NK, P_SIZE, P_SIZE), P_SIZE ** -0.5, 0.375, ((0, 8),)),
        "coarse_of": with_ends(jax.random.randint(seeds[2], (NK,), 0, NKC), jax.random.fold_in(seeds[2], 1), 0, NKC - 1).astype(jnp.int32),
        "energy": jnp.clip(jnp.exp(math.log(8.0) - 2.0794415 * jax.random.uniform(seeds[3], (HAM,), jnp.float32) ** level_of(seeds[3], (HAM,), ((0, 16),), -0.2, 0.2)), 1.0, 8.0),
        "start_vectors": noise(seeds[4], (HAM, VECS), 1.0, 6.0, ((0, 128),), jnp.float32),
    }


newton_turns = 8

def inverse_root(gram):
    size = gram.shape[0]
    identity = jnp.eye(size, dtype=jnp.float32)
    scale_norm = jnp.sqrt(jnp.sum(gram * gram))
    ymat = gram / scale_norm
    zmat = identity
    for turn_index in range(newton_turns):
        middle = 1.5 * identity - 0.5 * jnp.dot(zmat, ymat, precision=lax.Precision.HIGHEST)
        ymat = jnp.dot(ymat, middle, precision=lax.Precision.HIGHEST)
        zmat = jnp.dot(middle, zmat, precision=lax.Precision.HIGHEST)
    return zmat / jnp.sqrt(scale_norm)

def reference(coarse_kernel, correlations, coarse_of, energy, start_vectors):
    rotations = correlations.astype(jnp.float32)
    width = correlations.shape[1]

    def one_row(carry, fine_index):
        strip = coarse_kernel[coarse_of[fine_index]].astype(jnp.float32)
        left_side = jnp.einsum('pa,bpq->baq', rotations[fine_index], strip).astype(jnp.bfloat16)
        picked = jnp.take(left_side, coarse_of, axis=0).astype(jnp.float32)
        tile_row = jnp.einsum('kpq,kqs->pks', picked, rotations).astype(jnp.bfloat16)
        return (carry, tile_row)
    total = NK * width
    carry_out, tiles = lax.scan(one_row, jnp.zeros((), jnp.float32), jnp.arange(NK, dtype=jnp.int32))
    matrix = tiles.reshape(total, total)
    current = start_vectors
    scale_col = energy[:, None]
    gram = jnp.zeros((current.shape[1], current.shape[1]), jnp.float32)
    for turn_index in range(STEPS):
        image = lax.dot_general(matrix, current.astype(jnp.bfloat16), (((0,), (0,)), ((), ())), preferred_element_type=jnp.float32)
        scaled = (image + scale_col * current) / scale_col
        gram = jnp.dot(scaled.T, scaled, precision=lax.Precision.HIGHEST)
        current = jnp.dot(scaled, inverse_root(gram), precision=lax.Precision.HIGHEST)
    return (matrix, current, gram)
```

```python
import functools

import jax
import jax.numpy as jnp
from jax import lax
from jax.experimental import pallas as pl
from jax.experimental.pallas import tpu as pltpu
from jax.sharding import PartitionSpec as P

STEPS = 2
TURNS = 8
F32 = jnp.float32
BF16 = jnp.bfloat16
MESH = pl.DeviceIdType.MESH
ANY = pl.ANY
VMEM = pltpu.VMEM
HIGHEST = lax.Precision.HIGHEST

COLOURS = (
    ((0, 192), "xyz"),
    ((192, 176), "yzx"),
    ((368, 144), "zxy"),
)
N_RING = 6


def place():
    row, col = lax.axis_index("row"), lax.axis_index("col")
    return {
        "x": lax.div(row, 4),
        "z": lax.rem(row, 4),
        "y": lax.div(col, 2),
        "h": lax.rem(col, 2),
    }


def device(at):
    return (at["x"] * 4 + at["z"], at["y"] * 2 + at["h"])


def moved(at, dim, by):
    return {**at, dim: lax.rem(at[dim] + by, 4)}


def gather_kernel(
    unit, corr, start, kall, crow, seg, own_sem, send, recv, dsend, drecv, csend, crecv, ssend, srecv, lsem
):
    me = place()
    row, col = lax.axis_index("row"), lax.axis_index("col")
    partner = {**me, "h": 1 - me["h"]}

    barrier = pltpu.get_barrier_semaphore()
    for dim in "xz":
        for by in (1, 3):
            pl.semaphore_signal(barrier, inc=1, device_id=device(moved(me, dim, by)), device_id_type=MESH)
    for by in range(1, 8):
        pl.semaphore_signal(barrier, inc=1, device_id=(row, lax.rem(col + by, 8)), device_id_type=MESH)
    pl.semaphore_wait(barrier, 11)

    def region(at, whole, rows):
        i = [pl.ds(0, 4) if d in whole else at[d] for d in "yxz"]
        return kall.at[i[0], at["h"], i[1], i[2], pl.ds(*rows), :]

    def halves(rows):
        first, n = rows
        return ((first, n // 2), (first + n // 2, n // 2))

    def copy(src, dst, pair, sems, to):
        return pltpu.make_async_remote_copy(
            src_ref=src,
            dst_ref=dst,
            send_sem=sems[0].at[pair],
            recv_sem=sems[1].at[pair],
            device_id=device(to),
            device_id_type=MESH,
        )

    pending = []

    class Ring:
        def __init__(self, number, dim, rows, whole, at, own=None):
            self.base = number * 6
            self.dim, self.rows, self.whole, self.at, self.own = dim, rows, whole, at, own

        def send(self, slot, at, rows, by, src=None):
            dst = region(at, self.whole, rows)
            c = copy(dst if src is None else src, dst, self.base + slot, (send, recv), moved(me, self.dim, by))
            c.start()
            pending.append(c)

        def got(self, slot, at, rows):
            dst = region(at, self.whole, rows)
            copy(dst, dst, self.base + slot, (send, recv), moved(me, self.dim, 1)).wait_recv()

        def part(self, rows):
            return None if self.own is None else self.own.at[pl.ds(*rows), :]

        def start(self):
            a, b = halves(self.rows)
            self.send(0, self.at, a, 1, self.part(a))
            self.send(1, self.at, b, 3, self.part(b))
            self.send(2, self.at, b, 1, self.part(b))
            self.send(3, self.at, a, 3, self.part(a))

        def forward(self):
            a, b = halves(self.rows)
            self.left, self.right = moved(self.at, self.dim, 3), moved(self.at, self.dim, 1)
            self.got(0, self.left, a)
            self.send(4, self.left, a, 1)
            self.got(1, self.right, b)
            self.send(5, self.right, b, 3)

        def sides(self):
            a, b = halves(self.rows)
            self.got(2, self.left, b)
            self.got(3, self.right, a)
            return (self.left, self.right)

        def far(self):
            a, b = halves(self.rows)
            at = moved(self.at, self.dim, 2)
            self.got(4, at, a)
            self.got(5, at, b)
            return at

    shared = []

    def share(at, whole, rows):
        r = region(at, whole, rows)
        c = copy(r, r, len(shared), (dsend, drecv), partner)
        c.start()
        shared.append((c, {**at, "h": partner["h"]}, whole, rows))

    mine = pltpu.make_async_copy(unit, kall.at[me["y"], me["h"], me["x"], me["z"]], own_sem)
    mine.start()
    rings = [[Ring(c * N_RING, o[0], rows, "", me, unit)] for c, (rows, o) in enumerate(COLOURS)]
    for (first,) in rings:
        first.start()
    unit_there = kall.at[me["y"], me["h"], me["x"], me["z"]]
    to_partner = copy(unit, unit_there, 54, (dsend, drecv), partner)
    to_partner.start()

    def start_copy(by, slot_col, to_col):
        return pltpu.make_async_remote_copy(
            src_ref=start,
            dst_ref=seg.at[slot_col],
            send_sem=ssend.at[by],
            recv_sem=srecv.at[by],
            device_id=(row, to_col),
            device_id_type=MESH,
        )

    seg_mine = pltpu.make_async_copy(start, seg.at[col], lsem.at[0])
    seg_mine.start()
    seg_sent = []
    for by in range(1, 8):
        c = start_copy(by, col, lax.rem(col + by, 8))
        c.start()
        seg_sent.append(c)

    root = lax.div(row, 2)
    offset = lax.rem(row, 2) * 8
    is_root = col == root

    def corr_copy(by, to_col):
        return pltpu.make_async_remote_copy(
            src_ref=corr.at[pl.ds(offset, 8)],
            dst_ref=crow,
            send_sem=csend.at[by],
            recv_sem=crecv,
            device_id=(row, to_col),
            device_id_type=MESH,
        )

    @pl.when(is_root)
    def _():
        c = pltpu.make_async_copy(corr.at[pl.ds(offset, 8)], crow, lsem.at[1])
        c.start()
        for by in range(1, 8):
            corr_copy(by, lax.rem(col + by, 8)).start()

    mine.wait()
    for (first,) in rings:
        first.forward()
    for c, ((rows, o), (first,)) in enumerate(zip(COLOURS, rings)):
        for at in first.sides():
            share(at, "", rows)
        share(first.far(), "", rows)
        second = Ring(c * N_RING + 1, o[1], rows, o[0], me)
        rings[c].append(second)
        second.start()
    for c, (rows, o) in enumerate(COLOURS):
        third = Ring(c * N_RING + 2, o[2], rows, o[0], me)
        rings[c].append(third)
        third.start()
    for r in rings:
        r[1].forward()
    for c, (rows, o) in enumerate(COLOURS):
        for n, at in enumerate(rings[c][1].sides()):
            share(at, o[0], rows)
            ring = Ring(c * N_RING + 3 + n, o[2], rows, o[0], at)
            rings[c].append(ring)
            ring.start()
    for r in rings:
        r[2].forward()
    for c, (rows, o) in enumerate(COLOURS):
        at = rings[c][1].far()
        share(at, o[0], rows)
        ring = Ring(c * N_RING + 5, o[2], rows, o[0], at)
        rings[c].append(ring)
        ring.start()
    for n in (3, 4):
        for r in rings:
            r[n].forward()
    for c, (rows, o) in enumerate(COLOURS):
        for at in rings[c][2].sides():
            share(at, o[0], rows)
        share(rings[c][2].far(), o[0], rows)
    for r in rings:
        r[5].forward()
    for n in (3, 4, 5):
        for c, (rows, o) in enumerate(COLOURS):
            for at in rings[c][n].sides():
                share(at, o[0], rows)
            share(rings[c][n].far(), o[0], rows)

    for c in pending:
        c.wait_send()
    to_partner.wait_send()
    other = kall.at[me["y"], partner["h"], me["x"], me["z"]]
    copy(other, other, 54, (dsend, drecv), partner).wait_recv()
    for n, (c, at, whole, rows) in enumerate(shared):
        c.wait_send()
        r = region(at, whole, rows)
        copy(r, r, n, (dsend, drecv), partner).wait_recv()
    seg_mine.wait()
    for by, c in enumerate(seg_sent, 1):
        c.wait_send()
        start_copy(by, lax.rem(col + 8 - by, 8), col).wait_recv()

    @pl.when(is_root)
    def _():
        pltpu.make_async_copy(corr.at[pl.ds(offset, 8)], crow, lsem.at[1]).wait()
        for by in range(1, 8):
            corr_copy(by, lax.rem(col + by, 8)).wait_send()

    @pl.when(jnp.logical_not(is_root))
    def _():
        corr_copy(1, col).wait_recv()


def gathered(unit, corr, start):
    dma = pltpu.SemaphoreType.DMA
    any_spec = pl.BlockSpec(memory_space=ANY)
    vmem_spec = pl.BlockSpec(memory_space=VMEM)
    return pl.pallas_call(
        gather_kernel,
        out_shape=(
            jax.ShapeDtypeStruct((4, 2, 4, 4, 512, 256), BF16),
            jax.ShapeDtypeStruct((8, 256, 256), BF16),
            jax.ShapeDtypeStruct((8, 64, 256), F32),
        ),
        in_specs=[vmem_spec, any_spec, vmem_spec],
        out_specs=(any_spec, any_spec, any_spec),
        scratch_shapes=[
            dma,
            dma((108,)),
            dma((108,)),
            dma((55,)),
            dma((55,)),
            dma((8,)),
            dma,
            dma((8,)),
            dma((8,)),
            dma((2,)),
        ],
        compiler_params=pltpu.CompilerParams(collective_id=0, has_side_effects=True),
        name="gather",
    )(unit, corr, start)


def tile_kernel(co, pos, *refs):
    blocks, (crow, corr, seg, ham, part, turned, segb) = refs[:8], refs[8:]

    @pl.when(pl.program_id(0) == 0)
    def _():
        for k in range(8):
            turned[k] = crow[k].T
        segb[...] = seg[...].astype(BF16)

    total = jnp.zeros((64, 256), F32)
    for k in range(8):
        left = jnp.dot(turned[k], blocks[k][...], preferred_element_type=F32).astype(BF16)
        tile = jnp.dot(left, corr[...], preferred_element_type=F32).astype(BF16)
        ham[k * 256 : (k + 1) * 256, :] = tile
        total += jnp.dot(segb[k], tile, preferred_element_type=F32)
    part[...] = total.astype(BF16)


def tiled(coarse_of, kall, crow, corr, seg):
    pos = jnp.stack([lax.axis_index("row") * 8, lax.axis_index("col") * 16]).astype(jnp.int32)

    def block(k):
        def index(m, co, pos):
            a, b = co[pos[0] + k], co[pos[1] + m]
            return (a // 4, (a // 2) % 2, b // 4, b % 4, a % 2, 0)

        return pl.BlockSpec((None, None, None, None, 256, 256), index)

    grid_spec = pltpu.PrefetchScalarGridSpec(
        num_scalar_prefetch=2,
        grid=(16,),
        in_specs=[block(k) for k in range(8)]
        + [
            pl.BlockSpec((8, 256, 256), lambda m, co, pos: (0, 0, 0)),
            pl.BlockSpec((None, 256, 256), lambda m, co, pos: (m, 0, 0)),
            pl.BlockSpec((8, 64, 256), lambda m, co, pos: (0, 0, 0)),
        ],
        out_specs=[
            pl.BlockSpec((2048, 256), lambda m, co, pos: (0, m)),
            pl.BlockSpec((None, 64, 256), lambda m, co, pos: (m, 0, 0)),
        ],
        scratch_shapes=[VMEM((8, 256, 256), BF16), VMEM((8, 64, 256), BF16)],
    )
    return pl.pallas_call(
        tile_kernel,
        grid_spec=grid_spec,
        out_shape=(
            jax.ShapeDtypeStruct((2048, 4096), BF16),
            jax.ShapeDtypeStruct((16, 64, 256), BF16),
        ),
        name="tiles",
    )(coarse_of, pos, *([kall] * 8), crow, corr, seg)


def split(x):
    high = x.astype(BF16)
    return high, (x - high.astype(F32)).astype(BF16)


def dot3(rotation, x):
    rh, rl = split(rotation.T)
    xh, xl = split(x)
    lhs = jnp.concatenate([rh, rl, rh], axis=1)
    rhs = jnp.concatenate([xh, xh, xl], axis=0)
    return jnp.dot(lhs, rhs, preferred_element_type=F32)


def inverse_root(gram):
    size = gram.shape[0]
    at = lax.broadcasted_iota(jnp.int32, (size, size), 0)
    identity = jnp.where(at == lax.broadcasted_iota(jnp.int32, (size, size), 1), 1.0, 0.0).astype(F32)
    norm = jnp.sqrt(jnp.sum(gram * gram))
    y = gram / norm
    z = identity
    for _ in range(TURNS):
        t = 1.5 * identity - 0.5 * jnp.dot(z, y, precision=HIGHEST, preferred_element_type=F32)
        y = jnp.dot(y, t, precision=HIGHEST, preferred_element_type=F32)
        z = jnp.dot(t, z, precision=HIGHEST, preferred_element_type=F32)
    return z / jnp.sqrt(norm)


def power_kernel(
    part, ham, energy, seg, vectors, gram_out,
    hamv, parts, image, rsbuf, agbuf, gbuf, gmine, cur, curb,
    hsem, rsend, rrecv, psend, precv, asend, arecv, gsend, grecv,
):
    row, col = lax.axis_index("row"), lax.axis_index("col")
    to_row, to_col = 2 * col + lax.div(row, 8), lax.rem(row, 8)
    own = 8 * row + col
    from_row, from_col = lax.rem(own, 16), lax.div(own, 16)
    moves = jnp.logical_or(to_row != row, to_col != col)

    barrier = pltpu.get_barrier_semaphore()
    for by in range(1, 16):
        pl.semaphore_signal(barrier, inc=1, device_id=(lax.rem(row + by, 16), col), device_id_type=MESH)
    for by in range(1, 8):
        pl.semaphore_signal(barrier, inc=1, device_id=(row, lax.rem(col + by, 8)), device_id_type=MESH)

    @pl.when(moves)
    def _():
        pl.semaphore_signal(barrier, inc=1, device_id=(to_row, to_col), device_id_type=MESH)
        pl.semaphore_signal(barrier, inc=1, device_id=(from_row, from_col), device_id_type=MESH)
        pl.semaphore_wait(barrier, 24)

    @pl.when(jnp.logical_not(moves))
    def _():
        pl.semaphore_wait(barrier, 22)

    fetch = pltpu.make_async_copy(ham, hamv, hsem)
    fetch.start()

    def remote(src, dst, s, r, to):
        return pltpu.make_async_remote_copy(
            src_ref=src, dst_ref=dst, send_sem=s, recv_sem=r, device_id=to, device_id_type=MESH
        )

    cur[...] = seg[...]
    inverse = 1.0 / energy[...]
    for step in range(STEPS):
        last = step == STEPS - 1
        outgoing = part if step == 0 else parts
        sent = []
        for by in range(1, 16):
            to = lax.rem(row + by, 16)
            if step > 0:
                columns = pl.ds(pl.multiple_of(to * 256, 256), 256)
                total = jnp.zeros((64, 256), F32)
                for k in range(8):
                    total += jnp.dot(curb[k], hamv[pl.ds(k * 256, 256), columns], preferred_element_type=F32)
                parts[by] = total.astype(BF16)
                src = parts.at[by]
            else:
                src = part.at[to]
            c = remote(src, rsbuf.at[step, by], rsend.at[step, by], rrecv.at[step, by], (to, col))
            c.start()
            sent.append(c)
        if step > 0:
            columns = pl.ds(pl.multiple_of(row * 256, 256), 256)
            total = jnp.zeros((64, 256), F32)
            for k in range(8):
                total += jnp.dot(curb[k], hamv[pl.ds(k * 256, 256), columns], preferred_element_type=F32)
        else:
            total = part[row].astype(F32)
        for by in range(1, 16):
            remote(
                rsbuf.at[step, by], rsbuf.at[step, by], rsend.at[step, by], rrecv.at[step, by], (row, col)
            ).wait_recv()
            total += rsbuf[step, by].astype(F32)
        image[step] = total.astype(BF16)

        @pl.when(moves)
        def _():
            c = remote(image.at[step], agbuf.at[step, to_col], psend.at[step], precv.at[step], (to_row, to_col))
            c.start()
            c.wait_send()
            remote(
                agbuf.at[step, col], agbuf.at[step, col], psend.at[step], precv.at[step], (row, col)
            ).wait_recv()

        @pl.when(jnp.logical_not(moves))
        def _():
            agbuf[step, col] = image[step]

        for by in range(1, 8):
            to = lax.rem(col + by, 8)
            c = remote(
                agbuf.at[step, col], agbuf.at[step, col], asend.at[step, by], arecv.at[step, by], (row, to)
            )
            c.start()
            sent.append(c)
        for by in range(1, 8):
            slot = lax.rem(col + 8 - by, 8)
            remote(
                agbuf.at[step, slot], agbuf.at[step, slot], asend.at[step, by], arecv.at[step, by], (row, col)
            ).wait_recv()
        square = jnp.zeros((128, 128), F32)
        for k in range(8):
            scaled = agbuf[step, k].astype(F32) * inverse[k : k + 1, :] + cur[k]
            cur[k] = scaled
            both = jnp.concatenate(split(scaled), axis=0)
            square += lax.dot_general(both, both, (((1,), (1,)), ((), ())), preferred_element_type=F32)
        own_gram = (square[:64, :64] + square[64:, 64:]) + (square[:64, 64:] + square[64:, :64])
        packed = jnp.concatenate([own_gram[:32], own_gram[32:]], axis=1)
        gmine[step] = packed
        gbuf[step, row] = packed
        for by in range(1, 16):
            to = lax.rem(row + by, 16)
            c = remote(gmine.at[step], gbuf.at[step, row], gsend.at[step, by], grecv.at[step, by], (to, col))
            c.start()
            sent.append(c)
        for by in range(1, 16):
            slot = lax.rem(row + 16 - by, 16)
            remote(
                gbuf.at[step, slot], gbuf.at[step, slot], gsend.at[step, by], grecv.at[step, by], (row, col)
            ).wait_recv()
        packed = gbuf[step, 0]
        for k in range(1, 16):
            packed += gbuf[step, k]
        gram = jnp.concatenate([packed[:, :64], packed[:, 64:]], axis=0)
        root = inverse_root(gram)
        if last:
            vectors[...] = dot3(root, cur[col])
            gram_out[...] = gram
        else:
            for k in range(8):
                turned = dot3(root, cur[k])
                cur[k] = turned
                curb[k] = turned.astype(BF16)
            fetch.wait()
        for c in sent:
            c.wait_send()


def powered(part, ham, energy, seg):
    dma = pltpu.SemaphoreType.DMA
    any_spec = pl.BlockSpec(memory_space=ANY)
    vmem_spec = pl.BlockSpec(memory_space=VMEM)
    return pl.pallas_call(
        power_kernel,
        out_shape=(jax.ShapeDtypeStruct((64, 256), F32), jax.ShapeDtypeStruct((64, 64), F32)),
        in_specs=[vmem_spec, any_spec, vmem_spec, vmem_spec],
        out_specs=(vmem_spec, vmem_spec),
        scratch_shapes=[
            VMEM((2048, 4096), BF16),
            VMEM((16, 64, 256), BF16),
            VMEM((STEPS, 64, 256), BF16),
            VMEM((STEPS, 16, 64, 256), BF16),
            VMEM((STEPS, 8, 64, 256), BF16),
            VMEM((STEPS, 16, 32, 128), F32),
            VMEM((STEPS, 32, 128), F32),
            VMEM((8, 64, 256), F32),
            VMEM((8, 64, 256), BF16),
            dma,
            dma((STEPS, 16)),
            dma((STEPS, 16)),
            dma((STEPS,)),
            dma((STEPS,)),
            dma((STEPS, 8)),
            dma((STEPS, 8)),
            dma((STEPS, 16)),
            dma((STEPS, 16)),
        ],
        compiler_params=pltpu.CompilerParams(
            collective_id=1, has_side_effects=True, vmem_limit_bytes=48 * 1024 * 1024
        ),
        name="power",
    )(part, ham, energy, seg)


def per_device(coarse_kernel, correlations, coarse_of, energy, start_vectors):
    unit = coarse_kernel.reshape(512, 256)
    kall, crow, seg = gathered(unit, correlations, start_vectors.T)
    ham, part = tiled(coarse_of, kall, crow, correlations, seg)
    vectors, gram = powered(part, ham, energy.reshape(8, 256), seg)
    return ham, vectors.T, gram


def solution(mesh):
    return jax.shard_map(
        per_device,
        mesh=mesh,
        in_specs=(
            P("col", "row", None, None),
            P("col", None, None),
            P(),
            P("row"),
            P(("row", "col"), None),
        ),
        out_specs=(P("row", "col"), P(("row", "col"), None), P()),
        check_vma=False,
    )
```

```python
import functools

import jax
import jax.numpy as jnp
from jax import lax
from jax.experimental import pallas as pl
from jax.experimental.pallas import tpu as pltpu
from jax.sharding import PartitionSpec as P

STEPS = 2
TURNS = 8
F32 = jnp.float32
BF16 = jnp.bfloat16
MESH = pl.DeviceIdType.MESH
ANY = pl.ANY
VMEM = pltpu.VMEM
HIGHEST = lax.Precision.HIGHEST

COLOURS = (
    ((0, 192), "xyz"),
    ((192, 176), "yzx"),
    ((368, 144), "zxy"),
)
N_RING = 6


def place():
    row, col = lax.axis_index("row"), lax.axis_index("col")
    return {
        "x": lax.div(row, 4),
        "z": lax.rem(row, 4),
        "y": lax.div(col, 2),
        "h": lax.rem(col, 2),
    }


def device(at):
    return (at["x"] * 4 + at["z"], at["y"] * 2 + at["h"])


def moved(at, dim, by):
    return {**at, dim: lax.rem(at[dim] + by, 4)}


def gather_kernel(
    unit, corr, start, kall, crow, seg, own_sem, send, recv, dsend, drecv, csend, crecv, ssend, srecv, lsem
):
    me = place()
    row, col = lax.axis_index("row"), lax.axis_index("col")
    partner = {**me, "h": 1 - me["h"]}

    barrier = pltpu.get_barrier_semaphore()
    for dim in "xz":
        for by in (1, 3):
            pl.semaphore_signal(barrier, inc=1, device_id=device(moved(me, dim, by)), device_id_type=MESH)
    for by in range(1, 8):
        pl.semaphore_signal(barrier, inc=1, device_id=(row, lax.rem(col + by, 8)), device_id_type=MESH)
    pl.semaphore_wait(barrier, 11)

    def region(at, whole, rows):
        i = [pl.ds(0, 4) if d in whole else at[d] for d in "yxz"]
        return kall.at[i[0], at["h"], i[1], i[2], pl.ds(*rows), :]

    def halves(rows):
        first, n = rows
        return ((first, n // 2), (first + n // 2, n // 2))

    def copy(src, dst, pair, sems, to):
        return pltpu.make_async_remote_copy(
            src_ref=src,
            dst_ref=dst,
            send_sem=sems[0].at[pair],
            recv_sem=sems[1].at[pair],
            device_id=device(to),
            device_id_type=MESH,
        )

    pending = []

    class Ring:
        def __init__(self, number, dim, rows, whole, at, own=None):
            self.base = number * 6
            self.dim, self.rows, self.whole, self.at, self.own = dim, rows, whole, at, own

        def send(self, slot, at, rows, by, src=None):
            dst = region(at, self.whole, rows)
            c = copy(dst if src is None else src, dst, self.base + slot, (send, recv), moved(me, self.dim, by))
            c.start()
            pending.append(c)

        def got(self, slot, at, rows):
            dst = region(at, self.whole, rows)
            copy(dst, dst, self.base + slot, (send, recv), moved(me, self.dim, 1)).wait_recv()

        def part(self, rows):
            return None if self.own is None else self.own.at[pl.ds(*rows), :]

        def start(self):
            a, b = halves(self.rows)
            self.send(0, self.at, a, 1, self.part(a))
            self.send(1, self.at, b, 3, self.part(b))
            self.send(2, self.at, b, 1, self.part(b))
            self.send(3, self.at, a, 3, self.part(a))

        def forward(self):
            a, b = halves(self.rows)
            self.left, self.right = moved(self.at, self.dim, 3), moved(self.at, self.dim, 1)
            self.got(0, self.left, a)
            self.send(4, self.left, a, 1)
            self.got(1, self.right, b)
            self.send(5, self.right, b, 3)

        def sides(self):
            a, b = halves(self.rows)
            self.got(2, self.left, b)
            self.got(3, self.right, a)
            return (self.left, self.right)

        def far(self):
            a, b = halves(self.rows)
            at = moved(self.at, self.dim, 2)
            self.got(4, at, a)
            self.got(5, at, b)
            return at

    shared = []

    def share(at, whole, rows):
        r = region(at, whole, rows)
        c = copy(r, r, len(shared), (dsend, drecv), partner)
        c.start()
        shared.append((c, {**at, "h": partner["h"]}, whole, rows))

    mine = pltpu.make_async_copy(unit, kall.at[me["y"], me["h"], me["x"], me["z"]], own_sem)
    mine.start()
    rings = [[Ring(c * N_RING, o[0], rows, "", me, unit)] for c, (rows, o) in enumerate(COLOURS)]
    for (first,) in rings:
        first.start()
    unit_there = kall.at[me["y"], me["h"], me["x"], me["z"]]
    to_partner = copy(unit, unit_there, 54, (dsend, drecv), partner)
    to_partner.start()

    def start_copy(by, slot_col, to_col):
        return pltpu.make_async_remote_copy(
            src_ref=start,
            dst_ref=seg.at[slot_col],
            send_sem=ssend.at[by],
            recv_sem=srecv.at[by],
            device_id=(row, to_col),
            device_id_type=MESH,
        )

    seg_mine = pltpu.make_async_copy(start, seg.at[col], lsem.at[0])
    seg_mine.start()
    seg_sent = []
    for by in range(1, 8):
        c = start_copy(by, col, lax.rem(col + by, 8))
        c.start()
        seg_sent.append(c)

    offset = lax.rem(row, 2) * 8
    away = lax.rem(me["y"] + 4 - me["x"], 4)
    on_line = me["h"] == lax.div(me["z"], 2)

    def corr_copy(n, first, to, src=crow):
        return pltpu.make_async_remote_copy(
            src_ref=src.at[pl.ds(first, 4)] if src is crow else src.at[pl.ds(offset + first, 4)],
            dst_ref=crow.at[pl.ds(first, 4)],
            send_sem=csend.at[n],
            recv_sem=crecv.at[n],
            device_id=device(to),
            device_id_type=MESH,
        )

    up, down = moved(me, "y", 1), moved(me, "y", 3)

    def corr_start():
        @pl.when(jnp.logical_and(on_line, away == 0))
        def _():
            pltpu.make_async_copy(corr.at[pl.ds(offset, 8)], crow, lsem.at[1]).start()
            corr_copy(0, 0, up, corr).start()
            corr_copy(1, 4, down, corr).start()
            corr_copy(2, 4, up, corr).start()
            corr_copy(3, 0, down, corr).start()
            corr_copy(4, 0, partner, corr).start()
            corr_copy(5, 4, partner, corr).start()

    def corr_forward():
        @pl.when(jnp.logical_and(on_line, away == 1))
        def _():
            corr_copy(0, 0, up).wait_recv()
            corr_copy(0, 0, up).start()
            corr_copy(4, 0, partner).start()
            corr_copy(2, 4, up).wait_recv()
            corr_copy(5, 4, partner).start()

        @pl.when(jnp.logical_and(on_line, away == 3))
        def _():
            corr_copy(1, 4, down).wait_recv()
            corr_copy(1, 4, down).start()
            corr_copy(5, 4, partner).start()
            corr_copy(3, 0, down).wait_recv()
            corr_copy(4, 0, partner).start()

    def corr_finish():
        @pl.when(jnp.logical_and(on_line, away == 0))
        def _():
            pltpu.make_async_copy(corr.at[pl.ds(offset, 8)], crow, lsem.at[1]).wait()
            for n, first in enumerate((0, 4, 4, 0)):
                corr_copy(n, first, up).wait_send()

        @pl.when(jnp.logical_and(on_line, away == 1))
        def _():
            corr_copy(0, 0, up).wait_send()

        @pl.when(jnp.logical_and(on_line, away == 3))
        def _():
            corr_copy(1, 4, up).wait_send()

        @pl.when(jnp.logical_and(on_line, away == 2))
        def _():
            corr_copy(0, 0, up).wait_recv()
            corr_copy(4, 0, partner).start()
            corr_copy(1, 4, down).wait_recv()
            corr_copy(5, 4, partner).start()

        @pl.when(on_line)
        def _():
            corr_copy(4, 0, partner).wait_send()
            corr_copy(5, 4, partner).wait_send()

        @pl.when(jnp.logical_not(on_line))
        def _():
            corr_copy(4, 0, partner).wait_recv()
            corr_copy(5, 4, partner).wait_recv()

    mine.wait()
    for (first,) in rings:
        first.forward()
    for c, ((rows, o), (first,)) in enumerate(zip(COLOURS, rings)):
        for at in first.sides():
            share(at, "", rows)
        share(first.far(), "", rows)
        second = Ring(c * N_RING + 1, o[1], rows, o[0], me)
        rings[c].append(second)
        second.start()
    for c, (rows, o) in enumerate(COLOURS):
        third = Ring(c * N_RING + 2, o[2], rows, o[0], me)
        rings[c].append(third)
        third.start()
    corr_start()
    for r in rings:
        r[1].forward()
    for c, (rows, o) in enumerate(COLOURS):
        for n, at in enumerate(rings[c][1].sides()):
            share(at, o[0], rows)
            ring = Ring(c * N_RING + 3 + n, o[2], rows, o[0], at)
            rings[c].append(ring)
            ring.start()
    for r in rings:
        r[2].forward()
    for c, (rows, o) in enumerate(COLOURS):
        at = rings[c][1].far()
        share(at, o[0], rows)
        ring = Ring(c * N_RING + 5, o[2], rows, o[0], at)
        rings[c].append(ring)
        ring.start()
    for n in (3, 4):
        for r in rings:
            r[n].forward()
    corr_forward()
    for c, (rows, o) in enumerate(COLOURS):
        for at in rings[c][2].sides():
            share(at, o[0], rows)
        share(rings[c][2].far(), o[0], rows)
    for r in rings:
        r[5].forward()
    for n in (3, 4, 5):
        for c, (rows, o) in enumerate(COLOURS):
            for at in rings[c][n].sides():
                share(at, o[0], rows)
            share(rings[c][n].far(), o[0], rows)

    for c in pending:
        c.wait_send()
    to_partner.wait_send()
    other = kall.at[me["y"], partner["h"], me["x"], me["z"]]
    copy(other, other, 54, (dsend, drecv), partner).wait_recv()
    for n, (c, at, whole, rows) in enumerate(shared):
        c.wait_send()
        r = region(at, whole, rows)
        copy(r, r, n, (dsend, drecv), partner).wait_recv()
    seg_mine.wait()
    for by, c in enumerate(seg_sent, 1):
        c.wait_send()
        start_copy(by, lax.rem(col + 8 - by, 8), col).wait_recv()

    corr_finish()


def gathered(unit, corr, start):
    dma = pltpu.SemaphoreType.DMA
    any_spec = pl.BlockSpec(memory_space=ANY)
    vmem_spec = pl.BlockSpec(memory_space=VMEM)
    return pl.pallas_call(
        gather_kernel,
        out_shape=(
            jax.ShapeDtypeStruct((4, 2, 4, 4, 512, 256), BF16),
            jax.ShapeDtypeStruct((8, 256, 256), BF16),
            jax.ShapeDtypeStruct((8, 64, 256), F32),
        ),
        in_specs=[vmem_spec, any_spec, vmem_spec],
        out_specs=(any_spec, any_spec, any_spec),
        scratch_shapes=[
            dma,
            dma((108,)),
            dma((108,)),
            dma((55,)),
            dma((55,)),
            dma((6,)),
            dma((6,)),
            dma((8,)),
            dma((8,)),
            dma((2,)),
        ],
        compiler_params=pltpu.CompilerParams(collective_id=0, has_side_effects=True),
        name="gather",
    )(unit, corr, start)


def tile_kernel(co, pos, *refs):
    blocks, (crow, corr, seg, ham, part, turned, segb, lefts) = refs[:8], refs[8:]

    @pl.when(pl.program_id(0) == 0)
    def _():
        for k in range(8):
            turned[k] = crow[k].T
            segb[:, k * 256 : (k + 1) * 256] = seg[k].astype(BF16)

    for k in range(8):
        left = jnp.dot(turned[k], blocks[k][...], preferred_element_type=F32)
        lefts[k * 256 : (k + 1) * 256, :] = left.astype(BF16)
    tile = jnp.dot(lefts[...], corr[...], preferred_element_type=F32).astype(BF16)
    ham[...] = tile
    part[...] = jnp.dot(segb[...], tile, preferred_element_type=F32).astype(BF16)


def tiled(coarse_of, kall, crow, corr, seg):
    pos = jnp.stack([lax.axis_index("row") * 8, lax.axis_index("col") * 16]).astype(jnp.int32)

    kall = kall.reshape(8, 16, 2, 256, 256)

    def block(k):
        def index(m, co, pos):
            a, b = co[pos[0] + k], co[pos[1] + m]
            return (lax.div(a, 2), b, lax.rem(a, 2), 0, 0)

        return pl.BlockSpec((None, None, None, 256, 256), index)

    grid_spec = pltpu.PrefetchScalarGridSpec(
        num_scalar_prefetch=2,
        grid=(16,),
        in_specs=[block(k) for k in range(8)]
        + [
            pl.BlockSpec((8, 256, 256), lambda m, co, pos: (0, 0, 0)),
            pl.BlockSpec((None, 256, 256), lambda m, co, pos: (m, 0, 0)),
            pl.BlockSpec((8, 64, 256), lambda m, co, pos: (0, 0, 0)),
        ],
        out_specs=[
            pl.BlockSpec((2048, 256), lambda m, co, pos: (0, m)),
            pl.BlockSpec((None, 64, 256), lambda m, co, pos: (m, 0, 0)),
        ],
        scratch_shapes=[VMEM((8, 256, 256), BF16), VMEM((64, 2048), BF16), VMEM((2048, 256), BF16)],
    )
    return pl.pallas_call(
        tile_kernel,
        grid_spec=grid_spec,
        out_shape=(
            jax.ShapeDtypeStruct((2048, 4096), BF16),
            jax.ShapeDtypeStruct((16, 64, 256), BF16),
        ),
        name="tiles",
    )(coarse_of, pos, *([kall] * 8), crow, corr, seg)


def split(x):
    high = x.astype(BF16)
    return high, (x - high.astype(F32)).astype(BF16)


def dot3(rotation, x):
    rh, rl = split(rotation.T)
    xh, xl = split(x)
    lhs = jnp.concatenate([rh, rl, rh], axis=1)
    rhs = jnp.concatenate([xh, xh, xl], axis=0)
    return jnp.dot(lhs, rhs, preferred_element_type=F32)


def inverse_root(gram):
    size = gram.shape[0]
    at = lax.broadcasted_iota(jnp.int32, (size, size), 0)
    identity = jnp.where(at == lax.broadcasted_iota(jnp.int32, (size, size), 1), 1.0, 0.0).astype(F32)
    norm = jnp.sqrt(jnp.sum(gram * gram))
    y = gram / norm
    z = identity
    for _ in range(TURNS):
        t = 1.5 * identity - 0.5 * jnp.dot(z, y, precision=HIGHEST, preferred_element_type=F32)
        y = jnp.dot(y, t, precision=HIGHEST, preferred_element_type=F32)
        z = jnp.dot(t, z, precision=HIGHEST, preferred_element_type=F32)
    return z / jnp.sqrt(norm)


def power_kernel(
    part, ham, energy, seg, vectors, gram_out,
    hamv, parts, image, rsbuf, agbuf, gbuf, gmine, cur, curb,
    hsem, rsend, rrecv, psend, precv, asend, arecv, gsend, grecv,
):
    row, col = lax.axis_index("row"), lax.axis_index("col")
    to_row, to_col = 2 * col + lax.div(row, 8), lax.rem(row, 8)
    own = 8 * row + col
    from_row, from_col = lax.rem(own, 16), lax.div(own, 16)
    moves = jnp.logical_or(to_row != row, to_col != col)

    barrier = pltpu.get_barrier_semaphore()
    for by in range(1, 16):
        pl.semaphore_signal(barrier, inc=1, device_id=(lax.rem(row + by, 16), col), device_id_type=MESH)
    for by in range(1, 8):
        pl.semaphore_signal(barrier, inc=1, device_id=(row, lax.rem(col + by, 8)), device_id_type=MESH)

    @pl.when(moves)
    def _():
        pl.semaphore_signal(barrier, inc=1, device_id=(to_row, to_col), device_id_type=MESH)
        pl.semaphore_signal(barrier, inc=1, device_id=(from_row, from_col), device_id_type=MESH)
        pl.semaphore_wait(barrier, 24)

    @pl.when(jnp.logical_not(moves))
    def _():
        pl.semaphore_wait(barrier, 22)

    fetch = pltpu.make_async_copy(ham, hamv, hsem)
    fetch.start()

    def remote(src, dst, s, r, to):
        return pltpu.make_async_remote_copy(
            src_ref=src, dst_ref=dst, send_sem=s, recv_sem=r, device_id=to, device_id_type=MESH
        )

    cur[...] = seg[...]
    inverse = 1.0 / energy[...]
    for step in range(STEPS):
        last = step == STEPS - 1
        outgoing = part if step == 0 else parts
        sent = []
        for by in range(1, 16):
            to = lax.rem(row + by, 16)
            if step > 0:
                columns = pl.ds(pl.multiple_of(to * 256, 256), 256)
                total = jnp.zeros((64, 256), F32)
                for k in range(8):
                    total += jnp.dot(curb[k], hamv[pl.ds(k * 256, 256), columns], preferred_element_type=F32)
                parts[by] = total.astype(BF16)
                src = parts.at[by]
            else:
                src = part.at[to]
            c = remote(src, rsbuf.at[step, by], rsend.at[step, by], rrecv.at[step, by], (to, col))
            c.start()
            sent.append(c)
        if step > 0:
            columns = pl.ds(pl.multiple_of(row * 256, 256), 256)
            total = jnp.zeros((64, 256), F32)
            for k in range(8):
                total += jnp.dot(curb[k], hamv[pl.ds(k * 256, 256), columns], preferred_element_type=F32)
        else:
            total = part[row].astype(F32)
        for by in range(1, 16):
            remote(
                rsbuf.at[step, by], rsbuf.at[step, by], rsend.at[step, by], rrecv.at[step, by], (row, col)
            ).wait_recv()
            total += rsbuf[step, by].astype(F32)
        image[step] = total.astype(BF16)

        @pl.when(moves)
        def _():
            c = remote(image.at[step], agbuf.at[step, to_col], psend.at[step], precv.at[step], (to_row, to_col))
            c.start()
            c.wait_send()
            remote(
                agbuf.at[step, col], agbuf.at[step, col], psend.at[step], precv.at[step], (row, col)
            ).wait_recv()

        @pl.when(jnp.logical_not(moves))
        def _():
            agbuf[step, col] = image[step]

        for by in range(1, 8):
            to = lax.rem(col + by, 8)
            c = remote(
                agbuf.at[step, col], agbuf.at[step, col], asend.at[step, by], arecv.at[step, by], (row, to)
            )
            c.start()
            sent.append(c)
        for by in range(1, 8):
            slot = lax.rem(col + 8 - by, 8)
            remote(
                agbuf.at[step, slot], agbuf.at[step, slot], asend.at[step, by], arecv.at[step, by], (row, col)
            ).wait_recv()
        square = jnp.zeros((128, 128), F32)
        for k in range(8):
            scaled = agbuf[step, k].astype(F32) * inverse[k : k + 1, :] + cur[k]
            cur[k] = scaled
            both = jnp.concatenate(split(scaled), axis=0)
            square += lax.dot_general(both, both, (((1,), (1,)), ((), ())), preferred_element_type=F32)
        own_gram = (square[:64, :64] + square[64:, 64:]) + (square[:64, 64:] + square[64:, :64])
        packed = jnp.concatenate([own_gram[:32], own_gram[32:]], axis=1)
        gmine[step] = packed
        gbuf[step, row] = packed
        for by in range(1, 16):
            to = lax.rem(row + by, 16)
            c = remote(gmine.at[step], gbuf.at[step, row], gsend.at[step, by], grecv.at[step, by], (to, col))
            c.start()
            sent.append(c)
        for by in range(1, 16):
            slot = lax.rem(row + 16 - by, 16)
            remote(
                gbuf.at[step, slot], gbuf.at[step, slot], gsend.at[step, by], grecv.at[step, by], (row, col)
            ).wait_recv()
        packed = gbuf[step, 0]
        for k in range(1, 16):
            packed += gbuf[step, k]
        gram = jnp.concatenate([packed[:, :64], packed[:, 64:]], axis=0)
        root = inverse_root(gram)
        if last:
            vectors[...] = dot3(root, cur[col])
            gram_out[...] = gram
        else:
            for k in range(8):
                turned = dot3(root, cur[k])
                cur[k] = turned
                curb[k] = turned.astype(BF16)
            fetch.wait()
        for c in sent:
            c.wait_send()


def powered(part, ham, energy, seg):
    dma = pltpu.SemaphoreType.DMA
    any_spec = pl.BlockSpec(memory_space=ANY)
    vmem_spec = pl.BlockSpec(memory_space=VMEM)
    return pl.pallas_call(
        power_kernel,
        out_shape=(jax.ShapeDtypeStruct((64, 256), F32), jax.ShapeDtypeStruct((64, 64), F32)),
        in_specs=[vmem_spec, any_spec, vmem_spec, vmem_spec],
        out_specs=(vmem_spec, vmem_spec),
        scratch_shapes=[
            VMEM((2048, 4096), BF16),
            VMEM((16, 64, 256), BF16),
            VMEM((STEPS, 64, 256), BF16),
            VMEM((STEPS, 16, 64, 256), BF16),
            VMEM((STEPS, 8, 64, 256), BF16),
            VMEM((STEPS, 16, 32, 128), F32),
            VMEM((STEPS, 32, 128), F32),
            VMEM((8, 64, 256), F32),
            VMEM((8, 64, 256), BF16),
            dma,
            dma((STEPS, 16)),
            dma((STEPS, 16)),
            dma((STEPS,)),
            dma((STEPS,)),
            dma((STEPS, 8)),
            dma((STEPS, 8)),
            dma((STEPS, 16)),
            dma((STEPS, 16)),
        ],
        compiler_params=pltpu.CompilerParams(
            collective_id=1, has_side_effects=True, vmem_limit_bytes=48 * 1024 * 1024
        ),
        name="power",
    )(part, ham, energy, seg)


def per_device(coarse_kernel, correlations, coarse_of, energy, start_vectors):
    unit = coarse_kernel.reshape(512, 256)
    kall, crow, seg = gathered(unit, correlations, start_vectors.T)
    ham, part = tiled(coarse_of, kall, crow, correlations, seg)
    vectors, gram = powered(part, ham, energy.reshape(8, 256), seg)
    return ham, vectors.T, gram


def solution(mesh):
    return jax.shard_map(
        per_device,
        mesh=mesh,
        in_specs=(
            P("col", "row", None, None),
            P("col", None, None),
            P(),
            P("row"),
            P(("row", "col"), None),
        ),
        out_specs=(P("row", "col"), P(("row", "col"), None), P()),
        check_vma=False,
    )
```

```python
import functools

import jax
import jax.numpy as jnp
from jax import lax
from jax.experimental import pallas as pl
from jax.experimental.pallas import tpu as pltpu
from jax.sharding import PartitionSpec as P

STEPS = 2
TURNS = 8
F32 = jnp.float32
BF16 = jnp.bfloat16
MESH = pl.DeviceIdType.MESH
ANY = pl.ANY
VMEM = pltpu.VMEM
HIGHEST = lax.Precision.HIGHEST

COLOURS = (
    ((0, 192), "xyz"),
    ((192, 176), "yzx"),
    ((368, 144), "zxy"),
)
N_RING = 6


def place():
    row, col = lax.axis_index("row"), lax.axis_index("col")
    return {
        "x": lax.div(row, 4),
        "z": lax.rem(row, 4),
        "y": lax.div(col, 2),
        "h": lax.rem(col, 2),
    }


def device(at):
    return (at["x"] * 4 + at["z"], at["y"] * 2 + at["h"])


def moved(at, dim, by):
    return {**at, dim: lax.rem(at[dim] + by, 4)}


def gather_kernel(
    unit, corr, start, kall, crow, seg, own_sem, send, recv, dsend, drecv, csend, crecv, ssend, srecv, lsem
):
    me = place()
    row, col = lax.axis_index("row"), lax.axis_index("col")
    partner = {**me, "h": 1 - me["h"]}

    barrier = pltpu.get_barrier_semaphore()
    for dim in "xz":
        for by in (1, 2, 3):
            pl.semaphore_signal(barrier, inc=1, device_id=device(moved(me, dim, by)), device_id_type=MESH)
    for by in range(1, 8):
        pl.semaphore_signal(barrier, inc=1, device_id=(row, lax.rem(col + by, 8)), device_id_type=MESH)
    pl.semaphore_wait(barrier, 13)

    def region(at, whole, rows):
        i = [pl.ds(0, 4) if d in whole else at[d] for d in "yxz"]
        return kall.at[i[0], at["h"], i[1], i[2], pl.ds(*rows), :]

    def halves(rows):
        first, n = rows
        return ((first, n // 2), (first + n // 2, n // 2))

    def copy(src, dst, pair, sems, to):
        return pltpu.make_async_remote_copy(
            src_ref=src,
            dst_ref=dst,
            send_sem=sems[0].at[pair],
            recv_sem=sems[1].at[pair],
            device_id=device(to),
            device_id_type=MESH,
        )

    pending = []

    class Ring:
        def __init__(self, number, dim, rows, whole, at, own=None):
            self.base = number * 6
            self.direct = own is not None
            self.dim, self.rows, self.whole, self.at, self.own = dim, rows, whole, at, own

        def send(self, slot, at, rows, by, src=None):
            dst = region(at, self.whole, rows)
            c = copy(dst if src is None else src, dst, self.base + slot, (send, recv), moved(me, self.dim, by))
            c.start()
            pending.append(c)

        def got(self, slot, at, rows):
            dst = region(at, self.whole, rows)
            copy(dst, dst, self.base + slot, (send, recv), moved(me, self.dim, 1)).wait_recv()

        def part(self, rows):
            return None if self.own is None else self.own.at[pl.ds(*rows), :]

        def start(self):
            a, b = halves(self.rows)
            if self.direct:
                self.send(0, self.at, self.rows, 2, self.part(self.rows))
                self.send(1, self.at, self.rows, 1, self.part(self.rows))
                self.send(2, self.at, self.rows, 3, self.part(self.rows))
                return
            self.send(0, self.at, a, 1, self.part(a))
            self.send(1, self.at, b, 3, self.part(b))
            self.send(2, self.at, b, 1, self.part(b))
            self.send(3, self.at, a, 3, self.part(a))

        def forward(self):
            if self.direct:
                self.left, self.right = moved(self.at, self.dim, 3), moved(self.at, self.dim, 1)
                self.got(1, self.left, self.rows)
                share(self.left, self.whole, self.rows)
                self.got(2, self.right, self.rows)
                share(self.right, self.whole, self.rows)
                return
            a, b = halves(self.rows)
            self.left, self.right = moved(self.at, self.dim, 3), moved(self.at, self.dim, 1)
            self.got(0, self.left, a)
            self.send(4, self.left, a, 1)
            share(self.left, self.whole, a)
            self.got(1, self.right, b)
            self.send(5, self.right, b, 3)
            share(self.right, self.whole, b)

        def sides(self):
            if self.direct:
                return (self.left, self.right)
            a, b = halves(self.rows)
            self.got(2, self.left, b)
            share(self.left, self.whole, b)
            self.got(3, self.right, a)
            share(self.right, self.whole, a)
            return (self.left, self.right)

        def far(self):
            a, b = halves(self.rows)
            at = moved(self.at, self.dim, 2)
            if self.direct:
                self.got(0, at, self.rows)
                share(at, self.whole, self.rows)
                return at
            self.got(4, at, a)
            share(at, self.whole, a)
            self.got(5, at, b)
            share(at, self.whole, b)
            return at

    shared = []

    def share(at, whole, rows):
        r = region(at, whole, rows)
        c = copy(r, r, len(shared), (dsend, drecv), partner)
        c.start()
        shared.append((c, {**at, "h": partner["h"]}, whole, rows))

    mine = pltpu.make_async_copy(unit, kall.at[me["y"], me["h"], me["x"], me["z"]], own_sem)
    mine.start()
    rings = [[Ring(c * N_RING, o[0], rows, "", me, unit)] for c, (rows, o) in enumerate(COLOURS)]
    for (first,) in rings:
        first.start()
    unit_there = kall.at[me["y"], me["h"], me["x"], me["z"]]
    to_partner = copy(unit, unit_there, 108, (dsend, drecv), partner)
    to_partner.start()

    def start_copy(by, slot_col, to_col):
        return pltpu.make_async_remote_copy(
            src_ref=start,
            dst_ref=seg.at[slot_col],
            send_sem=ssend.at[by],
            recv_sem=srecv.at[by],
            device_id=(row, to_col),
            device_id_type=MESH,
        )

    seg_mine = pltpu.make_async_copy(start, seg.at[col], lsem.at[0])
    seg_mine.start()
    seg_sent = []
    for by in range(1, 8):
        c = start_copy(by, col, lax.rem(col + by, 8))
        c.start()
        seg_sent.append(c)

    offset = lax.rem(row, 2) * 8
    away = lax.rem(me["y"] + 4 - me["x"], 4)
    on_line = me["h"] == lax.div(me["z"], 2)

    def corr_copy(n, first, to, src=crow):
        return pltpu.make_async_remote_copy(
            src_ref=src.at[pl.ds(first, 4)] if src is crow else src.at[pl.ds(offset + first, 4)],
            dst_ref=crow.at[pl.ds(first, 4)],
            send_sem=csend.at[n],
            recv_sem=crecv.at[n],
            device_id=device(to),
            device_id_type=MESH,
        )

    up, down = moved(me, "y", 1), moved(me, "y", 3)

    def corr_start():
        @pl.when(jnp.logical_and(on_line, away == 0))
        def _():
            pltpu.make_async_copy(corr.at[pl.ds(offset, 8)], crow, lsem.at[1]).start()
            corr_copy(0, 0, up, corr).start()
            corr_copy(1, 4, down, corr).start()
            corr_copy(2, 4, up, corr).start()
            corr_copy(3, 0, down, corr).start()
            corr_copy(4, 0, partner, corr).start()
            corr_copy(5, 4, partner, corr).start()

    def corr_forward():
        @pl.when(jnp.logical_and(on_line, away == 1))
        def _():
            corr_copy(0, 0, up).wait_recv()
            corr_copy(0, 0, up).start()
            corr_copy(4, 0, partner).start()
            corr_copy(2, 4, up).wait_recv()
            corr_copy(5, 4, partner).start()

        @pl.when(jnp.logical_and(on_line, away == 3))
        def _():
            corr_copy(1, 4, down).wait_recv()
            corr_copy(1, 4, down).start()
            corr_copy(5, 4, partner).start()
            corr_copy(3, 0, down).wait_recv()
            corr_copy(4, 0, partner).start()

    def corr_finish():
        @pl.when(jnp.logical_and(on_line, away == 0))
        def _():
            pltpu.make_async_copy(corr.at[pl.ds(offset, 8)], crow, lsem.at[1]).wait()
            for n, first in enumerate((0, 4, 4, 0)):
                corr_copy(n, first, up).wait_send()

        @pl.when(jnp.logical_and(on_line, away == 1))
        def _():
            corr_copy(0, 0, up).wait_send()

        @pl.when(jnp.logical_and(on_line, away == 3))
        def _():
            corr_copy(1, 4, up).wait_send()

        @pl.when(jnp.logical_and(on_line, away == 2))
        def _():
            corr_copy(0, 0, up).wait_recv()
            corr_copy(4, 0, partner).start()
            corr_copy(1, 4, down).wait_recv()
            corr_copy(5, 4, partner).start()

        @pl.when(on_line)
        def _():
            corr_copy(4, 0, partner).wait_send()
            corr_copy(5, 4, partner).wait_send()

        @pl.when(jnp.logical_not(on_line))
        def _():
            corr_copy(4, 0, partner).wait_recv()
            corr_copy(5, 4, partner).wait_recv()

    mine.wait()
    for (first,) in rings:
        first.forward()
    for c, ((rows, o), (first,)) in enumerate(zip(COLOURS, rings)):
        first.sides()
        first.far()
        second = Ring(c * N_RING + 1, o[1], rows, o[0], me)
        rings[c].append(second)
        second.start()
    for c, (rows, o) in enumerate(COLOURS):
        third = Ring(c * N_RING + 2, o[2], rows, o[0], me)
        rings[c].append(third)
        third.start()
    corr_start()
    for r in rings:
        r[1].forward()
    for c, (rows, o) in enumerate(COLOURS):
        for n, at in enumerate(rings[c][1].sides()):
            ring = Ring(c * N_RING + 3 + n, o[2], rows, o[0], at)
            rings[c].append(ring)
            ring.start()
    for r in rings:
        r[2].forward()
    for r in rings:
        r[2].sides()
    for c, (rows, o) in enumerate(COLOURS):
        at = rings[c][1].far()
        ring = Ring(c * N_RING + 5, o[2], rows, o[0], at)
        rings[c].append(ring)
        ring.start()
    for n in (3, 4):
        for r in rings:
            r[n].forward()
        for r in rings:
            r[n].sides()
    corr_forward()
    for r in rings:
        r[2].far()
    for r in rings:
        r[5].forward()
    for r in rings:
        r[5].sides()
    for n in (3, 4, 5):
        for r in rings:
            r[n].far()

    for c in pending:
        c.wait_send()
    to_partner.wait_send()
    other = kall.at[me["y"], partner["h"], me["x"], me["z"]]
    copy(other, other, 108, (dsend, drecv), partner).wait_recv()
    for n, (c, at, whole, rows) in enumerate(shared):
        c.wait_send()
        r = region(at, whole, rows)
        copy(r, r, n, (dsend, drecv), partner).wait_recv()
    seg_mine.wait()
    for by, c in enumerate(seg_sent, 1):
        c.wait_send()
        start_copy(by, lax.rem(col + 8 - by, 8), col).wait_recv()

    corr_finish()


def gathered(unit, corr, start):
    dma = pltpu.SemaphoreType.DMA
    any_spec = pl.BlockSpec(memory_space=ANY)
    vmem_spec = pl.BlockSpec(memory_space=VMEM)
    return pl.pallas_call(
        gather_kernel,
        out_shape=(
            jax.ShapeDtypeStruct((4, 2, 4, 4, 512, 256), BF16),
            jax.ShapeDtypeStruct((8, 256, 256), BF16),
            jax.ShapeDtypeStruct((8, 64, 256), F32),
        ),
        in_specs=[vmem_spec, any_spec, vmem_spec],
        out_specs=(any_spec, any_spec, any_spec),
        scratch_shapes=[
            dma,
            dma((108,)),
            dma((108,)),
            dma((109,)),
            dma((109,)),
            dma((6,)),
            dma((6,)),
            dma((8,)),
            dma((8,)),
            dma((2,)),
        ],
        compiler_params=pltpu.CompilerParams(collective_id=0, has_side_effects=True),
        name="gather",
    )(unit, corr, start)


def tile_kernel(co, pos, *refs):
    blocks, (crow, corr, seg, ham, part, turned, segb, lefts) = refs[:8], refs[8:]

    @pl.when(pl.program_id(0) == 0)
    def _():
        for k in range(8):
            turned[k] = crow[k].T
            segb[:, k * 256 : (k + 1) * 256] = seg[k].astype(BF16)

    for k in range(8):
        left = jnp.dot(turned[k], blocks[k][...], preferred_element_type=F32)
        lefts[k * 256 : (k + 1) * 256, :] = left.astype(BF16)
    tile = jnp.dot(lefts[...], corr[...], preferred_element_type=F32).astype(BF16)
    ham[...] = tile
    part[...] = jnp.dot(segb[...], tile, preferred_element_type=F32).astype(BF16)


def tiled(coarse_of, kall, crow, corr, seg):
    pos = jnp.stack([lax.axis_index("row") * 8, lax.axis_index("col") * 16]).astype(jnp.int32)

    kall = kall.reshape(8, 16, 2, 256, 256)

    def block(k):
        def index(m, co, pos):
            a, b = co[pos[0] + k], co[pos[1] + m]
            return (lax.div(a, 2), b, lax.rem(a, 2), 0, 0)

        return pl.BlockSpec((None, None, None, 256, 256), index)

    grid_spec = pltpu.PrefetchScalarGridSpec(
        num_scalar_prefetch=2,
        grid=(16,),
        in_specs=[block(k) for k in range(8)]
        + [
            pl.BlockSpec((8, 256, 256), lambda m, co, pos: (0, 0, 0)),
            pl.BlockSpec((None, 256, 256), lambda m, co, pos: (m, 0, 0)),
            pl.BlockSpec((8, 64, 256), lambda m, co, pos: (0, 0, 0)),
        ],
        out_specs=[
            pl.BlockSpec((2048, 256), lambda m, co, pos: (0, m)),
            pl.BlockSpec((None, 64, 256), lambda m, co, pos: (m, 0, 0)),
        ],
        scratch_shapes=[VMEM((8, 256, 256), BF16), VMEM((64, 2048), BF16), VMEM((2048, 256), BF16)],
    )
    return pl.pallas_call(
        tile_kernel,
        grid_spec=grid_spec,
        out_shape=(
            jax.ShapeDtypeStruct((2048, 4096), BF16),
            jax.ShapeDtypeStruct((16, 64, 256), BF16),
        ),
        name="tiles",
    )(coarse_of, pos, *([kall] * 8), crow, corr, seg)


def split(x):
    high = x.astype(BF16)
    return high, (x - high.astype(F32)).astype(BF16)


def dot3(rotation, x):
    rh, rl = split(rotation.T)
    xh, xl = split(x)
    lhs = jnp.concatenate([rh, rl, rh], axis=1)
    rhs = jnp.concatenate([xh, xh, xl], axis=0)
    return jnp.dot(lhs, rhs, preferred_element_type=F32)


def inverse_root(gram):
    size = gram.shape[0]
    at = lax.broadcasted_iota(jnp.int32, (size, size), 0)
    identity = jnp.where(at == lax.broadcasted_iota(jnp.int32, (size, size), 1), 1.0, 0.0).astype(F32)
    norm = jnp.sqrt(jnp.sum(gram * gram))
    y = gram / norm
    z = identity
    for _ in range(TURNS):
        t = 1.5 * identity - 0.5 * jnp.dot(z, y, precision=HIGHEST, preferred_element_type=F32)
        y = jnp.dot(y, t, precision=HIGHEST, preferred_element_type=F32)
        z = jnp.dot(t, z, precision=HIGHEST, preferred_element_type=F32)
    return z / jnp.sqrt(norm)


def power_kernel(
    part, ham, energy, seg, vectors, gram_out,
    hamv, parts, image, rsbuf, agbuf, gbuf, gmine, cur, curb,
    hsem, rsend, rrecv, psend, precv, asend, arecv, gsend, grecv,
):
    row, col = lax.axis_index("row"), lax.axis_index("col")
    x, z, y, h = lax.div(row, 4), lax.rem(row, 4), lax.div(col, 2), lax.rem(col, 2)

    def block_of(at_row):
        to_y = lax.rem(2 * y + 6 - lax.div(at_row, 4), 4)
        turn = lax.rem(lax.rem(at_row, 4) + 4 - 2 * h, 4)
        return 8 * lax.rem(lax.div(turn + 1, 2), 2) + 2 * to_y + lax.div(turn, 2)

    mine = block_of(row)
    to_row, to_col = 2 * col + lax.div(mine, 8), lax.rem(mine, 8)
    low = lax.rem(z, 2)
    from_z = lax.rem(2 * lax.div(z, 2) + low + h * (2 * low - 1) + 4, 4)
    from_row, from_col = 4 * lax.rem(2 * x + 6 - y, 4) + from_z, 2 * x + lax.div(z, 2)

    barrier = pltpu.get_barrier_semaphore()
    for by in range(1, 16):
        pl.semaphore_signal(barrier, inc=1, device_id=(lax.rem(row + by, 16), col), device_id_type=MESH)
    for by in range(1, 8):
        pl.semaphore_signal(barrier, inc=1, device_id=(row, lax.rem(col + by, 8)), device_id_type=MESH)
    pl.semaphore_signal(barrier, inc=1, device_id=(to_row, to_col), device_id_type=MESH)
    pl.semaphore_signal(barrier, inc=1, device_id=(from_row, from_col), device_id_type=MESH)
    pl.semaphore_wait(barrier, 24)

    fetch = pltpu.make_async_copy(ham, hamv, hsem)
    fetch.start()

    def remote(src, dst, s, r, to):
        return pltpu.make_async_remote_copy(
            src_ref=src, dst_ref=dst, send_sem=s, recv_sem=r, device_id=to, device_id_type=MESH
        )

    cur[...] = seg[...]
    inverse = 1.0 / energy[...]
    for step in range(STEPS):
        last = step == STEPS - 1
        sent = []
        for by in range(1, 16):
            to = lax.rem(row + by, 16)
            if step > 0:
                columns = pl.ds(pl.multiple_of(block_of(to) * 256, 256), 256)
                total = jnp.zeros((64, 256), F32)
                for k in range(8):
                    total += jnp.dot(curb[k], hamv[pl.ds(k * 256, 256), columns], preferred_element_type=F32)
                parts[by] = total.astype(BF16)
                src = parts.at[by]
            else:
                src = part.at[block_of(to)]
            c = remote(src, rsbuf.at[step, by], rsend.at[step, by], rrecv.at[step, by], (to, col))
            c.start()
            sent.append(c)
        if step > 0:
            columns = pl.ds(pl.multiple_of(mine * 256, 256), 256)
            total = jnp.zeros((64, 256), F32)
            for k in range(8):
                total += jnp.dot(curb[k], hamv[pl.ds(k * 256, 256), columns], preferred_element_type=F32)
        else:
            total = part[mine].astype(F32)
        for by in range(1, 16):
            remote(
                rsbuf.at[step, by], rsbuf.at[step, by], rsend.at[step, by], rrecv.at[step, by], (row, col)
            ).wait_recv()
            total += rsbuf[step, by].astype(F32)
        image[step] = total.astype(BF16)

        c = remote(image.at[step], agbuf.at[step, to_col], psend.at[step], precv.at[step], (to_row, to_col))
        c.start()
        sent.append(c)
        remote(agbuf.at[step, col], agbuf.at[step, col], psend.at[step], precv.at[step], (row, col)).wait_recv()
        for by in range(1, 8):
            to = lax.rem(col + by, 8)
            c = remote(
                agbuf.at[step, col], agbuf.at[step, col], asend.at[step, by], arecv.at[step, by], (row, to)
            )
            c.start()
            sent.append(c)
        for by in range(1, 8):
            slot = lax.rem(col + 8 - by, 8)
            remote(
                agbuf.at[step, slot], agbuf.at[step, slot], asend.at[step, by], arecv.at[step, by], (row, col)
            ).wait_recv()
        square = jnp.zeros((128, 128), F32)
        for k in range(8):
            scaled = agbuf[step, k].astype(F32) * inverse[k : k + 1, :] + cur[k]
            cur[k] = scaled
            both = jnp.concatenate(split(scaled), axis=0)
            square += lax.dot_general(both, both, (((1,), (1,)), ((), ())), preferred_element_type=F32)
        own_gram = (square[:64, :64] + square[64:, 64:]) + (square[:64, 64:] + square[64:, :64])
        packed = jnp.concatenate([own_gram[:32], own_gram[32:]], axis=1)
        gmine[step] = packed
        gbuf[step, row] = packed
        for by in range(1, 16):
            to = lax.rem(row + by, 16)
            c = remote(gmine.at[step], gbuf.at[step, row], gsend.at[step, by], grecv.at[step, by], (to, col))
            c.start()
            sent.append(c)
        for by in range(1, 16):
            slot = lax.rem(row + 16 - by, 16)
            remote(
                gbuf.at[step, slot], gbuf.at[step, slot], gsend.at[step, by], grecv.at[step, by], (row, col)
            ).wait_recv()
        packed = gbuf[step, 0]
        for k in range(1, 16):
            packed += gbuf[step, k]
        gram = jnp.concatenate([packed[:, :64], packed[:, 64:]], axis=0)
        root = inverse_root(gram)
        if last:
            vectors[...] = dot3(root, cur[col])
            gram_out[...] = gram
        else:
            for k in range(8):
                turned = dot3(root, cur[k])
                cur[k] = turned
                curb[k] = turned.astype(BF16)
            fetch.wait()
        for c in sent:
            c.wait_send()


def powered(part, ham, energy, seg):
    dma = pltpu.SemaphoreType.DMA
    any_spec = pl.BlockSpec(memory_space=ANY)
    vmem_spec = pl.BlockSpec(memory_space=VMEM)
    return pl.pallas_call(
        power_kernel,
        out_shape=(jax.ShapeDtypeStruct((64, 256), F32), jax.ShapeDtypeStruct((64, 64), F32)),
        in_specs=[vmem_spec, any_spec, vmem_spec, vmem_spec],
        out_specs=(vmem_spec, vmem_spec),
        scratch_shapes=[
            VMEM((2048, 4096), BF16),
            VMEM((16, 64, 256), BF16),
            VMEM((STEPS, 64, 256), BF16),
            VMEM((STEPS, 16, 64, 256), BF16),
            VMEM((STEPS, 8, 64, 256), BF16),
            VMEM((STEPS, 16, 32, 128), F32),
            VMEM((STEPS, 32, 128), F32),
            VMEM((8, 64, 256), F32),
            VMEM((8, 64, 256), BF16),
            dma,
            dma((STEPS, 16)),
            dma((STEPS, 16)),
            dma((STEPS,)),
            dma((STEPS,)),
            dma((STEPS, 8)),
            dma((STEPS, 8)),
            dma((STEPS, 16)),
            dma((STEPS, 16)),
        ],
        compiler_params=pltpu.CompilerParams(
            collective_id=1, has_side_effects=True, vmem_limit_bytes=48 * 1024 * 1024
        ),
        name="power",
    )(part, ham, energy, seg)


def per_device(coarse_kernel, correlations, coarse_of, energy, start_vectors):
    unit = coarse_kernel.reshape(512, 256)
    kall, crow, seg = gathered(unit, correlations, start_vectors.T)
    ham, part = tiled(coarse_of, kall, crow, correlations, seg)
    vectors, gram = powered(part, ham, energy.reshape(8, 256), seg)
    return ham, vectors.T, gram


def solution(mesh):
    return jax.shard_map(
        per_device,
        mesh=mesh,
        in_specs=(
            P("col", "row", None, None),
            P("col", None, None),
            P(),
            P("row"),
            P(("row", "col"), None),
        ),
        out_specs=(P("row", "col"), P(("row", "col"), None), P()),
        check_vma=False,
    )
```

```python
import functools

import jax
import jax.numpy as jnp
from jax import lax
from jax.experimental import pallas as pl
from jax.experimental.pallas import tpu as pltpu
from jax.sharding import PartitionSpec as P

STEPS = 2
TURNS = 8
F32 = jnp.float32
BF16 = jnp.bfloat16
MESH = pl.DeviceIdType.MESH
ANY = pl.ANY
VMEM = pltpu.VMEM
HIGHEST = lax.Precision.HIGHEST

COLOURS = (
    ((0, 192), "xyz"),
    ((192, 192), "yzx"),
    ((384, 128), "zxy"),
)
N_RING = 6


def place():
    row, col = lax.axis_index("row"), lax.axis_index("col")
    return {
        "x": lax.div(row, 4),
        "z": lax.rem(row, 4),
        "y": lax.div(col, 2),
        "h": lax.rem(col, 2),
    }


def device(at):
    return (at["x"] * 4 + at["z"], at["y"] * 2 + at["h"])


def moved(at, dim, by):
    return {**at, dim: lax.rem(at[dim] + by, 4)}


def gather_kernel(
    unit, corr, start, kall, crow, seg, own_sem, send, recv, dsend, drecv, csend, crecv, ssend, srecv, lsem
):
    me = place()
    row, col = lax.axis_index("row"), lax.axis_index("col")
    partner = {**me, "h": 1 - me["h"]}

    barrier = pltpu.get_barrier_semaphore()
    for dim in "xz":
        for by in (1, 2, 3):
            pl.semaphore_signal(barrier, inc=1, device_id=device(moved(me, dim, by)), device_id_type=MESH)
    for by in range(1, 8):
        pl.semaphore_signal(barrier, inc=1, device_id=(row, lax.rem(col + by, 8)), device_id_type=MESH)
    pl.semaphore_wait(barrier, 13)

    def region(at, whole, rows):
        i = [pl.ds(0, 4) if d in whole else at[d] for d in "yxz"]
        return kall.at[i[0], at["h"], i[1], i[2], pl.ds(*rows), :]

    def halves(rows):
        first, n = rows
        return ((first, n // 2), (first + n // 2, n // 2))

    def copy(src, dst, pair, sems, to):
        return pltpu.make_async_remote_copy(
            src_ref=src,
            dst_ref=dst,
            send_sem=sems[0].at[pair],
            recv_sem=sems[1].at[pair],
            device_id=device(to),
            device_id_type=MESH,
        )

    pending = []

    class Ring:
        def __init__(self, number, dim, rows, whole, at, own=None):
            self.base = number * 6
            self.direct = own is not None
            self.dim, self.rows, self.whole, self.at, self.own = dim, rows, whole, at, own

        def send(self, slot, at, rows, by, src=None):
            dst = region(at, self.whole, rows)
            c = copy(dst if src is None else src, dst, self.base + slot, (send, recv), moved(me, self.dim, by))
            c.start()
            pending.append(c)

        def got(self, slot, at, rows):
            dst = region(at, self.whole, rows)
            copy(dst, dst, self.base + slot, (send, recv), moved(me, self.dim, 1)).wait_recv()

        def part(self, rows):
            return None if self.own is None else self.own.at[pl.ds(*rows), :]

        def start(self):
            a, b = halves(self.rows)
            if self.direct:
                self.send(0, self.at, self.rows, 2, self.part(self.rows))
                self.send(1, self.at, self.rows, 1, self.part(self.rows))
                self.send(2, self.at, self.rows, 3, self.part(self.rows))
                return
            self.send(0, self.at, a, 1, self.part(a))
            self.send(1, self.at, b, 3, self.part(b))
            self.send(2, self.at, b, 1, self.part(b))
            self.send(3, self.at, a, 3, self.part(a))

        def forward(self):
            if self.direct:
                self.left, self.right = moved(self.at, self.dim, 3), moved(self.at, self.dim, 1)
                self.got(1, self.left, self.rows)
                share(self.left, self.whole, self.rows)
                self.got(2, self.right, self.rows)
                share(self.right, self.whole, self.rows)
                return
            a, b = halves(self.rows)
            self.left, self.right = moved(self.at, self.dim, 3), moved(self.at, self.dim, 1)
            self.got(0, self.left, a)
            self.send(4, self.left, a, 1)
            share(self.left, self.whole, a)
            self.got(1, self.right, b)
            self.send(5, self.right, b, 3)
            share(self.right, self.whole, b)

        def sides(self):
            if self.direct:
                return (self.left, self.right)
            a, b = halves(self.rows)
            self.got(2, self.left, b)
            share(self.left, self.whole, b)
            self.got(3, self.right, a)
            share(self.right, self.whole, a)
            return (self.left, self.right)

        def far(self):
            a, b = halves(self.rows)
            at = moved(self.at, self.dim, 2)
            if self.direct:
                self.got(0, at, self.rows)
                share(at, self.whole, self.rows)
                return at
            self.got(4, at, a)
            share(at, self.whole, a)
            self.got(5, at, b)
            share(at, self.whole, b)
            return at

    shared = []

    def share(at, whole, rows):
        r = region(at, whole, rows)
        c = copy(r, r, len(shared), (dsend, drecv), partner)
        c.start()
        shared.append((c, {**at, "h": partner["h"]}, whole, rows))

    mine = pltpu.make_async_copy(unit, kall.at[me["y"], me["h"], me["x"], me["z"]], own_sem)
    mine.start()
    rings = [[Ring(c * N_RING, o[0], rows, "", me, unit)] for c, (rows, o) in enumerate(COLOURS)]
    for (first,) in rings:
        first.start()
    unit_there = kall.at[me["y"], me["h"], me["x"], me["z"]]
    to_partner = copy(unit, unit_there, 108, (dsend, drecv), partner)
    to_partner.start()

    def start_copy(by, slot_col, to_col):
        return pltpu.make_async_remote_copy(
            src_ref=start,
            dst_ref=seg.at[slot_col],
            send_sem=ssend.at[by],
            recv_sem=srecv.at[by],
            device_id=(row, to_col),
            device_id_type=MESH,
        )

    seg_mine = pltpu.make_async_copy(start, seg.at[col], lsem.at[0])
    seg_mine.start()
    seg_sent = []
    for by in range(1, 8):
        c = start_copy(by, col, lax.rem(col + by, 8))
        c.start()
        seg_sent.append(c)

    offset = lax.rem(row, 2) * 8
    away = lax.rem(me["y"] + 4 - me["x"], 4)
    on_line = me["h"] == lax.div(me["z"], 2)

    def corr_copy(n, first, to, src=crow):
        return pltpu.make_async_remote_copy(
            src_ref=src.at[pl.ds(first, 4)] if src is crow else src.at[pl.ds(offset + first, 4)],
            dst_ref=crow.at[pl.ds(first, 4)],
            send_sem=csend.at[n],
            recv_sem=crecv.at[n],
            device_id=device(to),
            device_id_type=MESH,
        )

    up, down = moved(me, "y", 1), moved(me, "y", 3)

    def corr_start():
        @pl.when(jnp.logical_and(on_line, away == 0))
        def _():
            pltpu.make_async_copy(corr.at[pl.ds(offset, 8)], crow, lsem.at[1]).start()
            corr_copy(0, 0, up, corr).start()
            corr_copy(1, 4, down, corr).start()
            corr_copy(2, 4, up, corr).start()
            corr_copy(3, 0, down, corr).start()
            corr_copy(4, 0, partner, corr).start()
            corr_copy(5, 4, partner, corr).start()

    def corr_forward():
        @pl.when(jnp.logical_and(on_line, away == 1))
        def _():
            corr_copy(0, 0, up).wait_recv()
            corr_copy(0, 0, up).start()
            corr_copy(4, 0, partner).start()
            corr_copy(2, 4, up).wait_recv()
            corr_copy(5, 4, partner).start()

        @pl.when(jnp.logical_and(on_line, away == 3))
        def _():
            corr_copy(1, 4, down).wait_recv()
            corr_copy(1, 4, down).start()
            corr_copy(5, 4, partner).start()
            corr_copy(3, 0, down).wait_recv()
            corr_copy(4, 0, partner).start()

    def corr_finish():
        @pl.when(jnp.logical_and(on_line, away == 0))
        def _():
            pltpu.make_async_copy(corr.at[pl.ds(offset, 8)], crow, lsem.at[1]).wait()
            for n, first in enumerate((0, 4, 4, 0)):
                corr_copy(n, first, up).wait_send()

        @pl.when(jnp.logical_and(on_line, away == 1))
        def _():
            corr_copy(0, 0, up).wait_send()

        @pl.when(jnp.logical_and(on_line, away == 3))
        def _():
            corr_copy(1, 4, up).wait_send()

        @pl.when(jnp.logical_and(on_line, away == 2))
        def _():
            corr_copy(0, 0, up).wait_recv()
            corr_copy(4, 0, partner).start()
            corr_copy(1, 4, down).wait_recv()
            corr_copy(5, 4, partner).start()

        @pl.when(on_line)
        def _():
            corr_copy(4, 0, partner).wait_send()
            corr_copy(5, 4, partner).wait_send()

        @pl.when(jnp.logical_not(on_line))
        def _():
            corr_copy(4, 0, partner).wait_recv()
            corr_copy(5, 4, partner).wait_recv()

    mine.wait()
    for (first,) in rings:
        first.forward()
    for c, ((rows, o), (first,)) in enumerate(zip(COLOURS, rings)):
        first.sides()
        first.far()
        second = Ring(c * N_RING + 1, o[1], rows, o[0], me)
        rings[c].append(second)
        second.start()
    for c, (rows, o) in enumerate(COLOURS):
        third = Ring(c * N_RING + 2, o[2], rows, o[0], me)
        rings[c].append(third)
        third.start()
    corr_start()
    for r in rings:
        r[1].forward()
    for c, (rows, o) in enumerate(COLOURS):
        for n, at in enumerate(rings[c][1].sides()):
            ring = Ring(c * N_RING + 3 + n, o[2], rows, o[0], at)
            rings[c].append(ring)
            ring.start()
    for r in rings:
        r[2].forward()
    for r in rings:
        r[2].sides()
    for c, (rows, o) in enumerate(COLOURS):
        at = rings[c][1].far()
        ring = Ring(c * N_RING + 5, o[2], rows, o[0], at)
        rings[c].append(ring)
        ring.start()
    for n in (3, 4):
        for r in rings:
            r[n].forward()
        for r in rings:
            r[n].sides()
    corr_forward()
    for r in rings:
        r[2].far()
    for r in rings:
        r[5].forward()
    for r in rings:
        r[5].sides()
    for n in (3, 4, 5):
        for r in rings:
            r[n].far()

    for c in pending:
        c.wait_send()
    to_partner.wait_send()
    other = kall.at[me["y"], partner["h"], me["x"], me["z"]]
    copy(other, other, 108, (dsend, drecv), partner).wait_recv()
    for n, (c, at, whole, rows) in enumerate(shared):
        c.wait_send()
        r = region(at, whole, rows)
        copy(r, r, n, (dsend, drecv), partner).wait_recv()
    seg_mine.wait()
    for by, c in enumerate(seg_sent, 1):
        c.wait_send()
        start_copy(by, lax.rem(col + 8 - by, 8), col).wait_recv()

    corr_finish()


def gathered(unit, corr, start):
    dma = pltpu.SemaphoreType.DMA
    any_spec = pl.BlockSpec(memory_space=ANY)
    vmem_spec = pl.BlockSpec(memory_space=VMEM)
    return pl.pallas_call(
        gather_kernel,
        out_shape=(
            jax.ShapeDtypeStruct((4, 2, 4, 4, 512, 256), BF16),
            jax.ShapeDtypeStruct((8, 256, 256), BF16),
            jax.ShapeDtypeStruct((8, 64, 256), F32),
        ),
        in_specs=[vmem_spec, any_spec, vmem_spec],
        out_specs=(any_spec, any_spec, any_spec),
        scratch_shapes=[
            dma,
            dma((108,)),
            dma((108,)),
            dma((109,)),
            dma((109,)),
            dma((6,)),
            dma((6,)),
            dma((8,)),
            dma((8,)),
            dma((2,)),
        ],
        compiler_params=pltpu.CompilerParams(collective_id=0, has_side_effects=True),
        name="gather",
    )(unit, corr, start)


def tile_kernel(co, pos, *refs):
    blocks, (crow, corr, seg, ham, part, turned, segb, lefts) = refs[:8], refs[8:]

    @pl.when(pl.program_id(0) == 0)
    def _():
        for k in range(8):
            turned[k] = crow[k].T
            segb[:, k * 256 : (k + 1) * 256] = seg[k].astype(BF16)

    for k in range(8):
        left = jnp.dot(turned[k], blocks[k][...], preferred_element_type=F32)
        lefts[k * 256 : (k + 1) * 256, :] = left.astype(BF16)
    tile = jnp.dot(lefts[...], corr[...], preferred_element_type=F32).astype(BF16)
    ham[...] = tile
    part[...] = jnp.dot(segb[...], tile, preferred_element_type=F32).astype(BF16)


def tiled(coarse_of, kall, crow, corr, seg):
    pos = jnp.stack([lax.axis_index("row") * 8, lax.axis_index("col") * 16]).astype(jnp.int32)

    kall = kall.reshape(8, 16, 2, 256, 256)

    def block(k):
        def index(m, co, pos):
            a, b = co[pos[0] + k], co[pos[1] + m]
            return (lax.div(a, 2), b, lax.rem(a, 2), 0, 0)

        return pl.BlockSpec((None, None, None, 256, 256), index)

    grid_spec = pltpu.PrefetchScalarGridSpec(
        num_scalar_prefetch=2,
        grid=(16,),
        in_specs=[block(k) for k in range(8)]
        + [
            pl.BlockSpec((8, 256, 256), lambda m, co, pos: (0, 0, 0)),
            pl.BlockSpec((None, 256, 256), lambda m, co, pos: (m, 0, 0)),
            pl.BlockSpec((8, 64, 256), lambda m, co, pos: (0, 0, 0)),
        ],
        out_specs=[
            pl.BlockSpec((2048, 256), lambda m, co, pos: (0, m)),
            pl.BlockSpec((None, 64, 256), lambda m, co, pos: (m, 0, 0)),
        ],
        scratch_shapes=[VMEM((8, 256, 256), BF16), VMEM((64, 2048), BF16), VMEM((2048, 256), BF16)],
    )
    return pl.pallas_call(
        tile_kernel,
        grid_spec=grid_spec,
        out_shape=(
            jax.ShapeDtypeStruct((2048, 4096), BF16),
            jax.ShapeDtypeStruct((16, 64, 256), BF16),
        ),
        name="tiles",
    )(coarse_of, pos, *([kall] * 8), crow, corr, seg)


def split(x):
    high = x.astype(BF16)
    return high, (x - high.astype(F32)).astype(BF16)


def dot3(rotation, x):
    rh, rl = split(rotation.T)
    xh, xl = split(x)
    lhs = jnp.concatenate([rh, rl, rh], axis=1)
    rhs = jnp.concatenate([xh, xh, xl], axis=0)
    return jnp.dot(lhs, rhs, preferred_element_type=F32)


def inverse_root(gram):
    size = gram.shape[0]
    at = lax.broadcasted_iota(jnp.int32, (size, size), 0)
    identity = jnp.where(at == lax.broadcasted_iota(jnp.int32, (size, size), 1), 1.0, 0.0).astype(F32)
    norm = jnp.sqrt(jnp.sum(gram * gram))
    y = gram / norm
    z = identity
    for _ in range(TURNS):
        t = 1.5 * identity - 0.5 * jnp.dot(z, y, precision=HIGHEST, preferred_element_type=F32)
        y = jnp.dot(y, t, precision=HIGHEST, preferred_element_type=F32)
        z = jnp.dot(t, z, precision=HIGHEST, preferred_element_type=F32)
    return z / jnp.sqrt(norm)


def power_kernel(
    part, ham, energy, seg, vectors, gram_out,
    hamv, parts, image, rsbuf, agbuf, gbuf, gmine, cur, curb,
    hsem, rsend, rrecv, psend, precv, asend, arecv, gsend, grecv,
):
    row, col = lax.axis_index("row"), lax.axis_index("col")
    x, z, y, h = lax.div(row, 4), lax.rem(row, 4), lax.div(col, 2), lax.rem(col, 2)

    def block_of(at_row):
        to_y = lax.rem(2 * y + 6 - lax.div(at_row, 4), 4)
        turn = lax.rem(lax.rem(at_row, 4) + 4 - 2 * h, 4)
        return 8 * lax.rem(lax.div(turn + 1, 2), 2) + 2 * to_y + lax.div(turn, 2)

    mine = block_of(row)
    to_row, to_col = 2 * col + lax.div(mine, 8), lax.rem(mine, 8)
    low = lax.rem(z, 2)
    from_z = lax.rem(2 * lax.div(z, 2) + low + h * (2 * low - 1) + 4, 4)
    from_row, from_col = 4 * lax.rem(2 * x + 6 - y, 4) + from_z, 2 * x + lax.div(z, 2)

    barrier = pltpu.get_barrier_semaphore()
    for by in range(1, 16):
        pl.semaphore_signal(barrier, inc=1, device_id=(lax.rem(row + by, 16), col), device_id_type=MESH)
    for by in range(1, 8):
        pl.semaphore_signal(barrier, inc=1, device_id=(row, lax.rem(col + by, 8)), device_id_type=MESH)
    pl.semaphore_signal(barrier, inc=1, device_id=(to_row, to_col), device_id_type=MESH)
    pl.semaphore_signal(barrier, inc=1, device_id=(from_row, from_col), device_id_type=MESH)
    pl.semaphore_wait(barrier, 24)

    fetch = pltpu.make_async_copy(ham, hamv, hsem)
    fetch.start()

    def remote(src, dst, s, r, to):
        return pltpu.make_async_remote_copy(
            src_ref=src, dst_ref=dst, send_sem=s, recv_sem=r, device_id=to, device_id_type=MESH
        )

    cur[...] = seg[...]
    inverse = 1.0 / energy[...]
    for step in range(STEPS):
        last = step == STEPS - 1
        sent = []
        for by in range(1, 16):
            to = lax.rem(row + by, 16)
            if step > 0:
                columns = pl.ds(pl.multiple_of(block_of(to) * 256, 256), 256)
                total = jnp.zeros((64, 256), F32)
                for k in range(8):
                    total += jnp.dot(curb[k], hamv[pl.ds(k * 256, 256), columns], preferred_element_type=F32)
                parts[by] = total.astype(BF16)
                src = parts.at[by]
            else:
                src = part.at[block_of(to)]
            c = remote(src, rsbuf.at[step, by], rsend.at[step, by], rrecv.at[step, by], (to, col))
            c.start()
            sent.append(c)
        if step > 0:
            columns = pl.ds(pl.multiple_of(mine * 256, 256), 256)
            total = jnp.zeros((64, 256), F32)
            for k in range(8):
                total += jnp.dot(curb[k], hamv[pl.ds(k * 256, 256), columns], preferred_element_type=F32)
        else:
            total = part[mine].astype(F32)
        for by in range(1, 16):
            remote(
                rsbuf.at[step, by], rsbuf.at[step, by], rsend.at[step, by], rrecv.at[step, by], (row, col)
            ).wait_recv()
            total += rsbuf[step, by].astype(F32)
        image[step] = total.astype(BF16)

        c = remote(image.at[step], agbuf.at[step, to_col], psend.at[step], precv.at[step], (to_row, to_col))
        c.start()
        sent.append(c)
        remote(agbuf.at[step, col], agbuf.at[step, col], psend.at[step], precv.at[step], (row, col)).wait_recv()
        for by in range(1, 8):
            to = lax.rem(col + by, 8)
            c = remote(
                agbuf.at[step, col], agbuf.at[step, col], asend.at[step, by], arecv.at[step, by], (row, to)
            )
            c.start()
            sent.append(c)
        for by in range(1, 8):
            slot = lax.rem(col + 8 - by, 8)
            remote(
                agbuf.at[step, slot], agbuf.at[step, slot], asend.at[step, by], arecv.at[step, by], (row, col)
            ).wait_recv()
        square = jnp.zeros((128, 128), F32)
        for k in range(8):
            scaled = agbuf[step, k].astype(F32) * inverse[k : k + 1, :] + cur[k]
            cur[k] = scaled
            both = jnp.concatenate(split(scaled), axis=0)
            square += lax.dot_general(both, both, (((1,), (1,)), ((), ())), preferred_element_type=F32)
        own_gram = (square[:64, :64] + square[64:, 64:]) + (square[:64, 64:] + square[64:, :64])
        packed = jnp.concatenate([own_gram[:32], own_gram[32:]], axis=1)
        gmine[step] = packed
        gbuf[step, row] = packed
        for by in range(1, 16):
            to = lax.rem(row + by, 16)
            c = remote(gmine.at[step], gbuf.at[step, row], gsend.at[step, by], grecv.at[step, by], (to, col))
            c.start()
            sent.append(c)
        for by in range(1, 16):
            slot = lax.rem(row + 16 - by, 16)
            remote(
                gbuf.at[step, slot], gbuf.at[step, slot], gsend.at[step, by], grecv.at[step, by], (row, col)
            ).wait_recv()
        packed = gbuf[step, 0]
        for k in range(1, 16):
            packed += gbuf[step, k]
        gram = jnp.concatenate([packed[:, :64], packed[:, 64:]], axis=0)
        root = inverse_root(gram)
        if last:
            vectors[...] = dot3(root, cur[col])
            gram_out[...] = gram
        else:
            for k in range(8):
                turned = dot3(root, cur[k])
                cur[k] = turned
                curb[k] = turned.astype(BF16)
            fetch.wait()
        for c in sent:
            c.wait_send()


def powered(part, ham, energy, seg):
    dma = pltpu.SemaphoreType.DMA
    any_spec = pl.BlockSpec(memory_space=ANY)
    vmem_spec = pl.BlockSpec(memory_space=VMEM)
    return pl.pallas_call(
        power_kernel,
        out_shape=(jax.ShapeDtypeStruct((64, 256), F32), jax.ShapeDtypeStruct((64, 64), F32)),
        in_specs=[vmem_spec, any_spec, vmem_spec, vmem_spec],
        out_specs=(vmem_spec, vmem_spec),
        scratch_shapes=[
            VMEM((2048, 4096), BF16),
            VMEM((16, 64, 256), BF16),
            VMEM((STEPS, 64, 256), BF16),
            VMEM((STEPS, 16, 64, 256), BF16),
            VMEM((STEPS, 8, 64, 256), BF16),
            VMEM((STEPS, 16, 32, 128), F32),
            VMEM((STEPS, 32, 128), F32),
            VMEM((8, 64, 256), F32),
            VMEM((8, 64, 256), BF16),
            dma,
            dma((STEPS, 16)),
            dma((STEPS, 16)),
            dma((STEPS,)),
            dma((STEPS,)),
            dma((STEPS, 8)),
            dma((STEPS, 8)),
            dma((STEPS, 16)),
            dma((STEPS, 16)),
        ],
        compiler_params=pltpu.CompilerParams(
            collective_id=1, has_side_effects=True, vmem_limit_bytes=48 * 1024 * 1024
        ),
        name="power",
    )(part, ham, energy, seg)


def per_device(coarse_kernel, correlations, coarse_of, energy, start_vectors):
    unit = coarse_kernel.reshape(512, 256)
    kall, crow, seg = gathered(unit, correlations, start_vectors.T)
    ham, part = tiled(coarse_of, kall, crow, correlations, seg)
    vectors, gram = powered(part, ham, energy.reshape(8, 256), seg)
    return ham, vectors.T, gram


def solution(mesh):
    return jax.shard_map(
        per_device,
        mesh=mesh,
        in_specs=(
            P("col", "row", None, None),
            P("col", None, None),
            P(),
            P("row"),
            P(("row", "col"), None),
        ),
        out_specs=(P("row", "col"), P(("row", "col"), None), P()),
        check_vma=False,
    )
```
